32 devices in a mesh: dp: 1 (over z), tp: 32 (over x, y, core).
Axes of the slice: x: 4, y: 4, z: 1, core: 2. Of those that a mesh axis runs over, the one named last changes fastest.
The devices are a block of a 4x4x8 slice.
Arguments:
- x: bfloat16 [8192, 4608], P(('dp', 'tp'))
- w_gate: bfloat16 [4608, 36864], P(None, 'tp')
- w_up: bfloat16 [4608, 36864], P(None, 'tp')
- w_down: bfloat16 [36864, 4608], P('tp')
Outputs:
- output: bfloat16 [8192, 4608], P(('dp', 'tp'))
All inputs are finite; a program needn't handle non-finite values.
Results may differ from the reference program's by a relative error of at most 0.016.
Values are sent between devices in bfloat16 or wider.
A program may use at most 768 MiB of HBM per device.

```python
import jax
import jax.numpy as jnp

ROWS = 8192
D = 4608
FF = 36864


def setup_inputs(seed: int = 0, part: int = 0) -> dict:
    kx, kg, ku, kd = jax.random.split(jax.random.key(seed), 4)
    drawn = {
        "x": jax.random.normal(jax.random.fold_in(kx, part), (ROWS, D), jnp.float32),
        "w_gate": jax.random.normal(kg, (D, FF), jnp.float32) * D**-0.5,
        "w_up": jax.random.normal(ku, (D, FF), jnp.float32) * D**-0.5,
        "w_down": jax.random.normal(kd, (FF, D), jnp.float32) * FF**-0.5,
    }
    return {k: v.astype(jnp.bfloat16) for k, v in drawn.items()}


def reference(x, w_gate, w_up, w_down):
    gate = jnp.dot(x, w_gate, preferred_element_type=jnp.float32)
    up = jnp.dot(x, w_up, preferred_element_type=jnp.float32)
    hidden = (jax.nn.gelu(gate) * up).astype(jnp.bfloat16)
    return jnp.dot(hidden, w_down, preferred_element_type=jnp.float32).astype(jnp.bfloat16)
```

```python
import functools
import math

import jax
import jax.numpy as jnp
from jax import lax
from jax.experimental import pallas as pl
from jax.experimental.pallas import tpu as pltpu
from jax.sharding import PartitionSpec as P

MESH = pl.DeviceIdType.MESH
BF16, F32 = jnp.bfloat16, jnp.float32
ANY = pl.BlockSpec(memory_space=pl.ANY)
LIMIT = 67043328

ORDER = (
    (0, 0), (0, -1), (0, 1), (-1, 0), (1, 0), (0, 2), (-1, -1), (1, -1),
    (-1, 1), (1, 1), (-1, 2), (1, 2), (2, 0), (2, 1), (2, -1), (2, 2),
)
SLOT = {place: i for i, place in enumerate(ORDER)}
SECOND_HALF = len(ORDER)


def pick(index, values):
    out = jnp.int32(values[0])
    for i, v in enumerate(values[1:], 1):
        out = jnp.where(index == i, jnp.int32(v), out)
    return out


class Place:
    def __init__(self, n):
        t = lax.axis_index("tp")
        self.n = n
        self.core = lax.rem(t, 2)
        self.partner = t + 1 - 2 * self.core
        self.y = lax.rem(lax.div(t, 2), n)
        self.x = lax.div(t, 2 * n)

    def gf(self, half, rg=0, rf=0):
        g, f = (self.x, self.y) if half == 0 else (self.y, self.x)
        return lax.rem(g + rg + self.n, self.n), lax.rem(f + rf + self.n, self.n)

    def device(self, half, rg, rf):
        g, f = self.gf(half, rg, rf)
        x, y = (g, f) if half == 0 else (f, g)
        return (x * self.n + y) * 2 + self.core


def remote(src, dst, send, recv, device):
    return pltpu.make_async_remote_copy(
        src_ref=src, dst_ref=dst, send_sem=send, recv_sem=recv, device_id={"tp": device}, device_id_type=MESH
    )


def greet(devices):
    barrier = pltpu.get_barrier_semaphore()
    for d in devices:
        pl.semaphore_signal(barrier, inc=1, device_id={"tp": d}, device_id_type=MESH)
    pl.semaphore_wait(barrier, len(devices))


def gather_kernel(
    n, x, wg, wu, wd, xg, hf, wdp,
    wv, xb, hb, send, recv, psend, precv, wsem, xsem, hsend, hlocal, hrecv, dsem,
):
    me = Place(n)
    c = me.core
    rows, depth = x.shape
    u = rows // 2
    units = wg.shape[1]
    tiles = units // 128

    def block(owner_core, half, rg, rf):
        g, f = me.gf(half, rg, rf)
        return xg.at[owner_core, half, g, f]

    counts = []

    def push(src, dst, half, device, slot):
        k = len(counts)
        counts.append(src)
        remote(src, dst, send.at[k], recv.at[half, slot], device).start()

    halves_sent = []

    def own(half):
        return x.at[pl.ds(half * u, u)]

    def forward(half, place):
        rg, rf = place
        mine = block(c, half, rg, rf)
        if place == (0, 0):
            src = own(half)
            push(src, mine, half, me.device(half, 0, 1), SLOT[(0, -1)])
            push(src, mine, half, me.device(half, 0, -1), SLOT[(0, 1)])
            push(src, mine, half, me.device(half, 1, 0), SLOT[(-1, 0)])
            push(src, mine, half, me.device(half, -1, 0), SLOT[(1, 0)])
        else:
            src = mine
        if place == (0, -1):
            part = mine.at[pl.ds(0, u // 2)]
            halves_sent.append(len(counts))
            push(part, part, half, me.device(half, 0, 1), SLOT[(0, 2)])
        if place == (0, 1):
            part = mine.at[pl.ds(u // 2, u // 2)]
            halves_sent.append(len(counts))
            push(part, part, half, me.device(half, 0, -1), SECOND_HALF)
        if rg == 0 and rf != 0:
            push(mine, mine, half, me.device(half, 1, 0), SLOT[(-1, rf)])
            push(mine, mine, half, me.device(half, -1, 0), SLOT[(1, rf)])
        if rg == -1 and rf in (0, -1):
            push(mine, mine, half, me.device(half, 1, 0), SLOT[(2, rf)])
        if rg == 1 and rf in (1, 2):
            push(mine, mine, half, me.device(half, -1, 0), SLOT[(2, rf)])
        remote(src, mine, psend.at[half, SLOT[place]], precv.at[half, SLOT[place]], me.partner).start()

    def arrived(half, place):
        mine = block(c, half, *place)
        if place == (0, 2):
            for slot, lo in ((SLOT[place], 0), (SECOND_HALF, u // 2)):
                part = mine.at[pl.ds(lo, u // 2)]
                remote(part, part, send.at[0], recv.at[half, slot], me.partner).wait_recv()
        else:
            remote(mine, mine, send.at[0], recv.at[half, SLOT[place]], me.partner).wait_recv()

    def handed_over(half, slot, rg, rf):
        theirs = block(1 - c, half, rg, rf)
        remote(theirs, theirs, send.at[0], precv.at[half, slot], me.partner).wait_recv()

    def tile_rows(core, half):
        return pl.ds(pl.multiple_of((core * 2 + half) * u, u), u)

    def tile_copy(slot, core, half, rg, rf):
        return pltpu.make_async_copy(
            block(core, half, rg, rf), xb.at[slot, tile_rows(core, half)], xsem.at[slot, core, half]
        )

    greet(
        [me.partner]
        + [me.device(0, rg, rf) for rg, rf in ((0, 1), (0, -1), (1, 0), (-1, 0))]
    )
    for half in (0, 1):
        forward(half, (0, 0))
    for half in (0, 1):
        pltpu.make_async_copy(own(half), xb.at[0, tile_rows(c, half)], xsem.at[0, c, half]).start()

    def weights(j, part):
        w = (wg, wu)[part]
        return pltpu.make_async_copy(
            w.at[:, pl.ds(pl.multiple_of(j * 128, 128), 128)],
            wv.at[j, :, pl.ds(part * 128, 128)],
            wsem.at[j, part],
        )

    def start_weights(j, carry):
        weights(j, 0).start()
        weights(j, 1).start()
        return carry

    lax.fori_loop(0, tiles, start_weights, 0)
    for half in (0, 1):
        handed_over(half, 0, 0, 0)
        tile_copy(0, 1 - c, half, 0, 0).start()
    down = remote(wd, wdp, dsem.at[0], dsem.at[1], me.partner)
    down.start()

    look, fetch = tiles // 3, (2 * tiles) // 3
    steps = len(ORDER)

    def offsets(s):
        return pick(s, [p[0] for p in ORDER]), pick(s, [p[1] for p in ORDER])

    def hidden_copies(slot, half, rg, rf):
        g, f = me.gf(half, rg, rf)
        mine = pltpu.make_async_copy(
            hb.at[slot, tile_rows(c, half)], hf.at[c, half, g, f], hlocal.at[slot, half]
        )
        theirs = remote(
            hb.at[slot, tile_rows(1 - c, half)], hf.at[c, half, g, f], hsend.at[slot, half], hrecv.at[0], me.partner
        )
        return mine, theirs

    def step(s, carry):
        slot = lax.rem(s, 2)
        rg, rf = offsets(s)
        ng, nf = offsets(s + 1)
        for core in (0, 1):
            for half in (0, 1):
                tile_copy(slot, core, half, rg, rf).wait()

        @pl.when(s >= 2)
        def _():
            for half in (0, 1):
                mine, theirs = hidden_copies(slot, half, rg, rf)
                mine.wait()
                theirs.wait_send()

        def tile(j, carry):
            @pl.when(s == 0)
            def _():
                weights(j, 0).wait()
                weights(j, 1).wait()

            @pl.when(j == look)
            def _():
                for k in range(1, steps):

                    @pl.when(s == k - 1)
                    def _():
                        for half in (0, 1):
                            arrived(half, ORDER[k])
                            forward(half, ORDER[k])

            @pl.when((j == fetch) & (s < steps - 1))
            def _():
                for half in (0, 1):
                    tile_copy(1 - slot, c, half, ng, nf).start()
                for half in (0, 1):
                    handed_over(half, s + 1, ng, nf)
                    tile_copy(1 - slot, 1 - c, half, ng, nf).start()

            both = jnp.dot(xb[slot], wv[j], preferred_element_type=F32)
            gate, up = both[:, :128], both[:, 128:]
            hb[slot, :, pl.ds(pl.multiple_of(j * 128, 128), 128)] = (jax.nn.gelu(gate) * up).astype(BF16)
            return carry

        lax.fori_loop(0, tiles, tile, 0)
        for half in (0, 1):
            mine, theirs = hidden_copies(slot, half, rg, rf)
            mine.start()
            theirs.start()
        return carry

    lax.fori_loop(0, steps, step, 0)

    for slot in (0, 1):
        for half in (0, 1):
            mine, theirs = hidden_copies(slot, half, 0, 0)
            mine.wait()
            theirs.wait_send()
    landed = hf.at[1 - c]
    remote(landed, landed, send.at[0], hrecv.at[0], me.partner).wait_recv()
    down.wait()
    for k in range(len(counts)):
        part = own(0).at[pl.ds(0, u // 2)] if k in halves_sent else own(0)
        remote(part, part, send.at[k], recv.at[0, 0], me.partner).wait_send()
    for half in (0, 1):
        for slot in range(steps):
            remote(own(half), own(half), psend.at[half, slot], recv.at[0, 0], me.partner).wait_send()


FAR = (2, 1, -1, 0)
STAGES = 4


def scatter_kernel(
    n, hf, wd, wdp, y, r0, r1, r2, r3,
    wv, hv, st, acc, a0, a1, wsem, hsem, ssem, s0, s1, s2, s3, q0, q1, asem, lsem,
):
    me = Place(n)
    c = me.core
    _, _, _, _, u, units = hf.shape
    h2 = u // 2
    depth = wd.shape[1]
    wide = math.gcd(depth, 512)
    tiles = depth // wide

    greet([me.device(0, rg, rf) for rg, rf in ((0, 1), (0, -1), (1, 0), (-1, 0))])

    def weights(core, src):
        return pltpu.make_async_copy(src, wv.at[pl.ds(pl.multiple_of(core * units, 128), units)], wsem.at[core])

    weights(c, wd).start()
    weights(1 - c, wdp).start()

    places = (
        [(2, df) for df in FAR]
        + [(dg, df) for df in FAR[:3] for dg in (1, -1)]
        + [(0, df) for df in FAR]
        + [(1, 0), (-1, 0)]
    )
    count = len(places)

    def hidden(t):
        dg, df = pick(t, [p[0] for p in places]), pick(t, [p[1] for p in places])
        out = []
        for half in (0, 1):
            g, f = me.gf(half, dg, df)
            for core in (0, 1):
                out.append(
                    pltpu.make_async_copy(
                        hf.at[core, half, g, f],
                        hv.at[lax.rem(t, 2), pl.ds(half * u, u), pl.ds(core * units, units)],
                        hsem.at[lax.rem(t, 2), half, core],
                    )
                )
        return out

    for copy in hidden(jnp.int32(0)):
        copy.start()
    weights(c, wd).wait()
    weights(1 - c, wdp).wait()

    def begin(t):
        for copy in hidden(t):
            copy.wait()

        @pl.when(t + 1 < count)
        def _():
            for copy in hidden(t + 1):
                copy.start()

    def columns(i):
        return pl.ds(pl.multiple_of(i * wide, wide), wide)

    def product(t, i):
        return jnp.dot(hv[lax.rem(t, 2)], wv[:, columns(i)], preferred_element_type=F32)

    def far_send(stage, half, side, fi):
        part = st.at[stage, pl.ds(half * u + side * h2, h2)]
        return remote(
            part, r0.at[half, side, fi], ssem.at[stage, half, side], q0.at[half, side, fi],
            me.device(half, 1 - 2 * side, 0),
        )

    def near_send(stage, half, side, fi):
        part = st.at[stage, pl.ds(half * u, u)]
        return remote(
            part, r1.at[half, side, fi], ssem.at[stage, half, 0], q1.at[half, side, fi],
            me.device(half, 1 - 2 * side, 0),
        )

    def level0(i, carry):
        begin(i)

        def tile(k, carry):
            st[i, :, columns(k)] = product(i, k).astype(BF16)
            return carry

        lax.fori_loop(0, tiles, tile, 0)
        for half in (0, 1):
            for side in (0, 1):
                far_send(i, half, side, i).start()
        return carry

    lax.fori_loop(0, 4, level0, 0)

    def fetch0(half, side, fi):
        return pltpu.make_async_copy(r0.at[half, side, fi], a0.at[side, half], asem.at[side, half])

    def level1(t, fi, stage0, previous):
        for side in (0, 1):
            stage = stage0 + side
            begin(t + side)
            for half in (0, 1):
                far_send(0, half, side, fi).wait_recv()
                fetch0(half, side, fi).start()
            previous(stage, side)
            for half in (0, 1):
                fetch0(half, side, fi).wait()

            def tile(k, carry):
                total = product(t + side, k)
                parts = []
                for half in (0, 1):
                    for piece in (0, 1):
                        lo = half * u + piece * h2
                        rows = total[lo : lo + h2]
                        if piece == side:
                            rows = rows + a0[side, half, :, columns(k)].astype(F32)
                        parts.append(rows.astype(BF16))
                st[stage, :, columns(k)] = jnp.concatenate(parts, axis=0)
                return carry

            lax.fori_loop(0, tiles, tile, 0)
            for half in (0, 1):
                near_send(stage, half, side, fi).start()

    def far_sent(stage, side):
        for half in (0, 1):
            for s in (0, 1):
                far_send(stage, half, s, 0).wait_send()

    def near_sent(stage, side):
        for half in (0, 1):
            near_send(stage, half, side, 0).wait_send()

    def level1_first(i, carry):
        level1(4 + 2 * i, i, 2 * i, far_sent)
        return carry

    lax.fori_loop(0, 2, level1_first, 0)
    level1(8, 2, 0, near_sent)

    def keep(i, carry):
        t = 10 + i
        begin(t)

        def tile(k, carry):
            acc[i, :, columns(k)] = product(t, k)
            return carry

        lax.fori_loop(0, tiles, tile, 0)
        return carry

    lax.fori_loop(0, 4, keep, 0)

    def add(which, sources):
        for i, (wait, landing, lo, size) in enumerate(sources):
            wait()
            pltpu.make_async_copy(landing, a1.at[i, pl.ds(0, size)], lsem.at[i]).start()
        for i, (wait, landing, lo, size) in enumerate(sources):
            pltpu.make_async_copy(landing, a1.at[i, pl.ds(0, size)], lsem.at[i]).wait()

            def some(k, carry, i=i, lo=lo):
                rows = pl.ds(pl.multiple_of(lo + k * 16, 16), 16)
                acc[which, rows] += a1[i, pl.ds(pl.multiple_of(k * 16, 16), 16)].astype(F32)
                return carry

            lax.fori_loop(0, size // 16, some, 0)

    def rounded(which, stage):
        def some(k, carry):
            rows = pl.ds(pl.multiple_of(k * 16, 16), 16)
            st[stage, rows] = acc[which, rows].astype(BF16)
            return carry

        lax.fori_loop(0, 2 * u // 16, some, 0)

    def from_near(fi):
        return [
            (near_send(0, half, side, fi).wait_recv, r1.at[half, side, fi], half * u, u)
            for half in (0, 1)
            for side in (0, 1)
        ]

    def turn_send(half, side):
        part = st.at[2, pl.ds(half * u + side * h2, h2)]
        return remote(part, r2.at[half, side], s2.at[half, side], s0.at[half, side], me.device(half, 0, 1 - 2 * side))

    def last_send(half, side):
        part = st.at[2 + side, pl.ds(half * u, u)]
        return remote(part, r3.at[half, side], s3.at[half, side], s1.at[half, side], me.device(half, 0, 1 - 2 * side))

    add(0, from_near(0))
    near_sent(2, 0)
    rounded(0, 2)
    for half in (0, 1):
        for side in (0, 1):
            turn_send(half, side).start()

    level1(14, 3, 0, near_sent)

    near_sent(3, 1)
    for side in (0, 1):
        add(1 + side, from_near(1 + side))
    for half in (0, 1):
        for side in (0, 1):
            turn_send(half, side).wait_send()
    for side in (0, 1):
        add(
            1 + side,
            [(turn_send(half, side).wait_recv, r2.at[half, side], half * u + side * h2, h2) for half in (0, 1)],
        )
        rounded(1 + side, 2 + side)
        for half in (0, 1):
            last_send(half, side).start()

    add(3, from_near(3))
    add(
        3,
        [
            (last_send(half, side).wait_recv, r3.at[half, side], half * u, u)
            for half in (0, 1)
            for side in (0, 1)
        ],
    )
    near_sent(0, 0)
    rounded(3, 0)
    out = pltpu.make_async_copy(st.at[0], y, lsem.at[0])
    out.start()
    near_sent(1, 1)
    for half in (0, 1):
        for side in (0, 1):
            last_send(half, side).wait_send()
    out.wait()


def solution(mesh):
    n = math.isqrt(mesh.shape["tp"] // 2)
    assert n == 4 and 2 * n * n == mesh.shape["tp"]

    def step(x, w_gate, w_up, w_down):
        rows, depth = x.shape
        units = w_gate.shape[1]
        u = rows // 2
        dma = pltpu.SemaphoreType.DMA
        like = jax.ShapeDtypeStruct
        _, hidden, other_down = pl.pallas_call(
            functools.partial(gather_kernel, n),
            out_shape=(
                like((2, 2, n, n, u, depth), BF16),
                like((2, 2, n, n, u, units), BF16),
                like(w_down.shape, BF16),
            ),
            in_specs=[ANY] * 4,
            out_specs=(ANY,) * 3,
            scratch_shapes=[
                pltpu.VMEM((units // 128, depth, 256), BF16),
                pltpu.VMEM((2, 4 * u, depth), BF16),
                pltpu.VMEM((2, 4 * u, units), BF16),
                dma((32,)),
                dma((2, 17)),
                dma((2, 16)),
                dma((2, 16)),
                dma((units // 128, 2)),
                dma((2, 2, 2)),
                dma((2, 2)),
                dma((2, 2)),
                dma((1,)),
                dma((2,)),
            ],
            compiler_params=pltpu.CompilerParams(
                collective_id=0, has_side_effects=True, vmem_limit_bytes=LIMIT
            ),
            name="gather",
        )(x, w_gate, w_up, w_down)
        y, *_ = pl.pallas_call(
            functools.partial(scatter_kernel, n),
            out_shape=(
                like((rows, depth), BF16),
                like((2, 2, 4, u // 2, depth), BF16),
                like((2, 2, 4, u, depth), BF16),
                like((2, 2, u // 2, depth), BF16),
                like((2, 2, u, depth), BF16),
            ),
            in_specs=[ANY] * 3,
            out_specs=(ANY,) * 5,
            scratch_shapes=[
                pltpu.VMEM((2 * units, depth), BF16),
                pltpu.VMEM((2, 2 * u, 2 * units), BF16),
                pltpu.VMEM((STAGES, 2 * u, depth), BF16),
                pltpu.VMEM((4, 2 * u, depth), F32),
                pltpu.VMEM((2, 2, u // 2, depth), BF16),
                pltpu.VMEM((4, u, depth), BF16),
                dma((2,)),
                dma((2, 2, 2)),
                dma((STAGES, 2, 2)),
                dma((2, 2)),
                dma((2, 2)),
                dma((2, 2)),
                dma((2, 2)),
                dma((2, 2, 4)),
                dma((2, 2, 4)),
                dma((2, 2)),
                dma((4,)),
            ],
            compiler_params=pltpu.CompilerParams(
                collective_id=1, has_side_effects=True, vmem_limit_bytes=LIMIT
            ),
            name="scatter",
        )(hidden, w_down, other_down)
        return y

    return jax.shard_map(
        step,
        mesh=mesh,
        in_specs=(P(("dp", "tp"), None), P(None, "tp"), P(None, "tp"), P("tp", None)),
        out_specs=P(("dp", "tp"), None),
        check_vma=False,
    )
```

```python
import functools
import math

import jax
import jax.numpy as jnp
from jax import lax
from jax.experimental import pallas as pl
from jax.experimental.pallas import tpu as pltpu
from jax.sharding import PartitionSpec as P

MESH = pl.DeviceIdType.MESH
BF16, F32 = jnp.bfloat16, jnp.float32
ANY = pl.BlockSpec(memory_space=pl.ANY)
LIMIT = 67043328

ORDER = (
    (0, 0), (0, -1), (0, 1), (-1, 0), (1, 0), (0, 2), (-1, -1), (1, -1),
    (-1, 1), (1, 1), (-1, 2), (1, 2), (2, 0), (2, 1), (2, -1), (2, 2),
)
SLOT = {place: i for i, place in enumerate(ORDER)}
SECOND_HALF = len(ORDER)


def pick(index, values):
    out = jnp.int32(values[0])
    for i, v in enumerate(values[1:], 1):
        out = jnp.where(index == i, jnp.int32(v), out)
    return out


class Place:
    def __init__(self, n):
        t = lax.axis_index("tp")
        self.n = n
        self.core = lax.rem(t, 2)
        self.partner = t + 1 - 2 * self.core
        self.y = lax.rem(lax.div(t, 2), n)
        self.x = lax.div(t, 2 * n)

    def gf(self, half, rg=0, rf=0):
        g, f = (self.x, self.y) if half == 0 else (self.y, self.x)
        return lax.rem(g + rg + self.n, self.n), lax.rem(f + rf + self.n, self.n)

    def device(self, half, rg, rf):
        g, f = self.gf(half, rg, rf)
        x, y = (g, f) if half == 0 else (f, g)
        return (x * self.n + y) * 2 + self.core


def remote(src, dst, send, recv, device):
    return pltpu.make_async_remote_copy(
        src_ref=src, dst_ref=dst, send_sem=send, recv_sem=recv, device_id={"tp": device}, device_id_type=MESH
    )


def greet(devices):
    barrier = pltpu.get_barrier_semaphore()
    for d in devices:
        pl.semaphore_signal(barrier, inc=1, device_id={"tp": d}, device_id_type=MESH)
    pl.semaphore_wait(barrier, len(devices))


EARLY = (0, 1)


def kernel(
    n, x, wg, wu, wd, y, xg, hf, r0, r1, r2, r3,
    wdv, hv, st, send, recv, psend, precv, wsem, xsem, hsend, hlocal, hrecv, dsem,
    hsem, ssem, q0, q1, q2, q3, lsem,
):
    me = Place(n)
    c = me.core
    rows, depth = x.shape
    u = rows // 2
    units = wg.shape[1]
    h2 = u // 2
    wide = math.gcd(depth, 512)

    def block(owner_core, half, rg, rf):
        g, f = me.gf(half, rg, rf)
        return xg.at[owner_core, half, g, f]

    counts = []

    def push(src, dst, half, device, slot):
        k = len(counts)
        counts.append(src)
        remote(src, dst, send.at[k], recv.at[half, slot], device).start()

    halves_sent = []

    def own(half):
        return x.at[pl.ds(half * u, u)]

    def forward(half, place):
        rg, rf = place
        mine = block(c, half, rg, rf)
        if place == (0, 0):
            src = own(half)
            push(src, mine, half, me.device(half, 0, 1), SLOT[(0, -1)])
            push(src, mine, half, me.device(half, 0, -1), SLOT[(0, 1)])
            push(src, mine, half, me.device(half, 1, 0), SLOT[(-1, 0)])
            push(src, mine, half, me.device(half, -1, 0), SLOT[(1, 0)])
        else:
            src = mine
        if place == (0, -1):
            part = mine.at[pl.ds(0, u // 2)]
            halves_sent.append(len(counts))
            push(part, part, half, me.device(half, 0, 1), SLOT[(0, 2)])
        if place == (0, 1):
            part = mine.at[pl.ds(u // 2, u // 2)]
            halves_sent.append(len(counts))
            push(part, part, half, me.device(half, 0, -1), SECOND_HALF)
        if rg == 0 and rf != 0:
            push(mine, mine, half, me.device(half, 1, 0), SLOT[(-1, rf)])
            push(mine, mine, half, me.device(half, -1, 0), SLOT[(1, rf)])
        if rg == -1 and rf in (0, -1):
            push(mine, mine, half, me.device(half, 1, 0), SLOT[(2, rf)])
        if rg == 1 and rf in (1, 2):
            push(mine, mine, half, me.device(half, -1, 0), SLOT[(2, rf)])
        remote(src, mine, psend.at[half, SLOT[place]], precv.at[half, SLOT[place]], me.partner).start()

    def arrived(half, place):
        mine = block(c, half, *place)
        if place == (0, 2):
            for slot, lo in ((SLOT[place], 0), (SECOND_HALF, u // 2)):
                part = mine.at[pl.ds(lo, u // 2)]
                remote(part, part, send.at[0], recv.at[half, slot], me.partner).wait_recv()
        else:
            remote(mine, mine, send.at[0], recv.at[half, SLOT[place]], me.partner).wait_recv()

    def handed_over(half, slot, rg, rf):
        theirs = block(1 - c, half, rg, rf)
        remote(theirs, theirs, send.at[0], precv.at[half, slot], me.partner).wait_recv()

    greet(
        [me.partner]
        + [me.device(0, rg, rf) for rg, rf in ((0, 1), (0, -1), (1, 0), (-1, 0))]
    )
    for half in (0, 1):
        forward(half, (0, 0))
    my_units = wdv.at[pl.ds(pl.multiple_of(c * units, 128), units)]
    down = remote(wd, my_units, dsem.at[0], dsem.at[1], me.partner)
    down_here = pltpu.make_async_copy(wd, my_units, dsem.at[2])

    def hidden(t, place):
        out = []
        for half in (0, 1):
            g, f = me.gf(half, *place)
            for core in (0, 1):
                out.append(
                    pltpu.make_async_copy(
                        hf.at[core, half, g, f],
                        hv.at[lax.rem(t, 2), pl.ds(half * u, u), pl.ds(core * units, units)],
                        hsem.at[lax.rem(t, 2), half, core],
                    )
                )
        return out

    def columns(i):
        return pl.ds(pl.multiple_of(i * wide, wide), wide)

    def product(t, i):
        return jnp.dot(hv[lax.rem(t, 2)], wdv[:, columns(i)], preferred_element_type=F32)

    def hidden_came(slot, rg, rf):
        for half in (0, 1):
            g, f = me.gf(half, rg, rf)
            landed = hf.at[1 - c, half, g, f]
            remote(landed, landed, send.at[0], hrecv.at[half, slot], me.partner).wait_recv()

    def over(body):
        def tile(k, carry):
            body(k)
            return carry

        lax.fori_loop(0, depth // wide, tile, 0)

    def to(half, dg, df):
        return me.device(half, df, dg)

    def far_send(ref, stage, half, side, fi):
        part = ref.at[pl.ds(half * u + side * h2, h2)]
        return remote(
            part, r0.at[half, side, fi], ssem.at[stage, half, side], q0.at[half, side, fi], to(half, 1 - 2 * side, 0)
        )

    def level0(ref, stage, t, fi):
        def body(k):
            ref[:, columns(k)] = product(t, k).astype(BF16)

        over(body)
        for half in (0, 1):
            for side in (0, 1):
                far_send(ref, stage, half, side, fi).start()

    def early_place(i):
        return pick(i, EARLY), 2

    def gather(wv, xb, hb):
        tiles = units // 128

        def tile_rows(core, half):
            return pl.ds(pl.multiple_of((core * 2 + half) * u, u), u)

        def tile_copy(slot, core, half, rg, rf):
            return pltpu.make_async_copy(
                block(core, half, rg, rf), xb.at[slot, tile_rows(core, half)], xsem.at[slot, core, half]
            )

        for half in (0, 1):
            pltpu.make_async_copy(own(half), xb.at[0, tile_rows(c, half)], xsem.at[0, c, half]).start()

        def weights(j, part):
            w = (wg, wu)[part]
            return pltpu.make_async_copy(
                w.at[:, pl.ds(pl.multiple_of(j * 128, 128), 128)],
                wv.at[j, :, pl.ds(part * 128, 128)],
                wsem.at[j, part],
            )

        def start_weights(j, carry):
            weights(j, 0).start()
            weights(j, 1).start()
            return carry

        lax.fori_loop(0, tiles, start_weights, 0)
        for half in (0, 1):
            handed_over(half, 0, 0, 0)
            tile_copy(0, 1 - c, half, 0, 0).start()
        down.start()
        down_here.start()

        group = math.gcd(tiles, 3)
        look, fetch = tiles // group // 3, 2 * (tiles // group) // 3
        steps = len(ORDER)

        def offsets(s):
            return pick(s, [p[0] for p in ORDER]), pick(s, [p[1] for p in ORDER])

        def hidden_copies(slot, half, rg, rf, s):
            g, f = me.gf(half, rg, rf)
            mine = pltpu.make_async_copy(
                hb.at[slot, tile_rows(c, half)], hf.at[c, half, g, f], hlocal.at[slot, half]
            )
            theirs = remote(
                hb.at[slot, tile_rows(1 - c, half)], hf.at[c, half, g, f],
                hsend.at[slot, half], hrecv.at[half, s], me.partner,
            )
            return mine, theirs

        def early_fetch(i):
            rg, rf = early_place(i)
            hidden_came(pick(i, [SLOT[(df, 2)] for df in EARLY]), rg, rf)
            for copy in hidden(i, (rg, rf)):
                copy.start()

        def step(s, carry):
            slot = lax.rem(s, 2)
            rg, rf = offsets(s)
            ng, nf = offsets(s + 1)
            for core in (0, 1):
                for half in (0, 1):
                    tile_copy(slot, core, half, rg, rf).wait()

            @pl.when(s >= 2)
            def _():
                for half in (0, 1):
                    mine, theirs = hidden_copies(slot, half, rg, rf, s)
                    mine.wait()
                    theirs.wait_send()

            def some_tiles(i, carry):
                @pl.when(s == 0)
                def _():
                    for q in range(group):
                        weights(i * group + q, 0).wait()
                        weights(i * group + q, 1).wait()

                @pl.when(i == look)
                def _():
                    for k in range(1, steps):

                        @pl.when(s == k - 1)
                        def _():
                            for half in (0, 1):
                                arrived(half, ORDER[k])
                                forward(half, ORDER[k])

                @pl.when(i == fetch)
                def _():
                    @pl.when(s < steps - 1)
                    def _():
                        for half in (0, 1):
                            tile_copy(1 - slot, c, half, ng, nf).start()
                        for half in (0, 1):
                            handed_over(half, s + 1, ng, nf)
                            tile_copy(1 - slot, 1 - c, half, ng, nf).start()

                    @pl.when(s == 11)
                    def _():
                        down.wait_recv()
                        down_here.wait()
                        early_fetch(jnp.int32(0))

                    @pl.when(s == 13)
                    def _():
                        early_fetch(jnp.int32(1))

                both = jnp.dot(xb[slot], wv[i * group], preferred_element_type=F32)
                for q in range(group):
                    gate, up = both[:, :128], both[:, 128:]
                    if q + 1 < group:
                        both = jnp.dot(xb[slot], wv[i * group + q + 1], preferred_element_type=F32)
                    j = i * group + q
                    hb[slot, :, pl.ds(pl.multiple_of(j * 128, 128), 128)] = (jax.nn.gelu(gate) * up).astype(BF16)
                return carry

            lax.fori_loop(0, tiles // group, some_tiles, 0)
            for half in (0, 1):
                mine, theirs = hidden_copies(slot, half, rg, rf, s)
                mine.start()
                theirs.start()

            def early(i, carry):
                for copy in hidden(i, early_place(i)):
                    copy.wait()

                level0(st.at[i], i, i, lax.rem(pick(i, EARLY) + n, n))
                return carry

            first = jnp.where(s == 13, 1, 0)
            lax.fori_loop(first, jnp.where(s == 13, 2, jnp.where(s == 11, 1, 0)), early, 0)
            return carry

        lax.fori_loop(0, steps, step, 0)
        for slot in (0, 1):
            for half in (0, 1):
                mine, theirs = hidden_copies(slot, half, 0, 0, 0)
                mine.wait()
                theirs.wait_send()

    pl.run_scoped(
        gather,
        pltpu.VMEM((units // 128, depth, 256), BF16),
        pltpu.VMEM((2, 4 * u, depth), BF16),
        pltpu.VMEM((2, 4 * u, units), BF16),
    )

    def scatter(acc, a0, a1, more):
        stages = [st.at[0], st.at[1], more.at[0], more.at[1], more.at[2]]
        near = (1, 2, -1, 0)
        places = (
            [(2, -1), (2, 2)]
            + [(dg, df) for df in near[:3] for dg in (1, -1)]
            + [(0, df) for df in (2, 1, -1, 0)]
            + [(1, 0), (-1, 0)]
        )
        done = {"t": 0}

        def fetch(i):
            dg, df = places[i]
            hidden_came(SLOT[(df, dg)], df, dg)
            for copy in hidden(jnp.int32(i + 1), (df, dg)):
                copy.start()

        fetch(0)

        def begin(place):
            i = done["t"]
            assert places[i] == place
            done["t"] = i + 1
            for copy in hidden(jnp.int32(i + 1), (place[1], place[0])):
                copy.wait()
            if i + 1 < len(places):
                fetch(i + 1)
            return jnp.int32(i + 1)

        pending = {
            i: [(lambda i=i, half=half, side=side: far_send(stages[i], i, half, side, 0)) for half in (0, 1) for side in (0, 1)]
            for i in range(4)
        }

        def free(stage):
            for copy in pending.pop(stage, []):
                copy().wait_send()

        for stage, df in ((2, -1), (3, 2)):
            t = begin((2, df))
            level0(stages[stage], stage, t, df % n)

        def near_send(stage, half, side, fi):
            part = stages[stage].at[pl.ds(half * u, u)]
            return remote(
                part, r1.at[half, side, fi], ssem.at[stage, half, 0], q1.at[half, side, fi], to(half, 1 - 2 * side, 0)
            )

        def level1(df, used):
            fi = df % n
            for side, stage in enumerate(used):
                t = begin((1 - 2 * side, df))
                fetches = []
                for half in (0, 1):
                    far_send(st.at[0], 0, half, side, fi).wait_recv()
                    copy = pltpu.make_async_copy(r0.at[half, side, fi], a0.at[half], lsem.at[half])
                    copy.start()
                    fetches.append(copy)
                free(stage)
                for copy in fetches:
                    copy.wait()

                def body(k, t=t, side=side, stage=stage):
                    total = product(t, k)
                    parts = []
                    for half in (0, 1):
                        for piece in (0, 1):
                            lo = half * u + piece * h2
                            rows = total[lo : lo + h2]
                            if piece == side:
                                rows = rows + a0[half, :, columns(k)].astype(F32)
                            parts.append(rows.astype(BF16))
                    stages[stage][:, columns(k)] = jnp.concatenate(parts, axis=0)

                over(body)
                for half in (0, 1):
                    near_send(stage, half, side, fi).start()
                pending[stage] = [
                    (lambda stage=stage, side=side, half=half: near_send(stage, half, side, 0)) for half in (0, 1)
                ]

        level1(1, (4, 0))
        level1(2, (1, 2))
        level1(-1, (3, 4))

        for i, df in enumerate((2, 1, -1, 0)):
            t = begin((0, df))

            def body(k, t=t, i=i):
                acc[i, :, columns(k)] = product(t, k)

            over(body)

        def add(which, sources):
            copies = []
            for i, (wait, landing, lo, size) in enumerate(sources):
                wait()
                copy = pltpu.make_async_copy(landing, a1.at[i, pl.ds(0, size)], lsem.at[i])
                copy.start()
                copies.append(copy)
            for i, (wait, landing, lo, size) in enumerate(sources):
                copies[i].wait()

                def some(k, carry, i=i, lo=lo):
                    rows = pl.ds(pl.multiple_of(lo + k * 16, 16), 16)
                    acc[which, rows] += a1[i, pl.ds(pl.multiple_of(k * 16, 16), 16)].astype(F32)
                    return carry

                lax.fori_loop(0, size // 16, some, 0)

        def rounded(which, stage):
            free(stage)

            def some(k, carry):
                rows = pl.ds(pl.multiple_of(k * 16, 16), 16)
                stages[stage][rows] = acc[which, rows].astype(BF16)
                return carry

            lax.fori_loop(0, 2 * u // 16, some, 0)

        def from_near(df):
            fi = df % n
            return [
                (near_send(0, half, side, fi).wait_recv, r1.at[half, side, fi], half * u, u)
                for half in (0, 1)
                for side in (0, 1)
            ]

        def turn_send(half, side):
            part = stages[0].at[pl.ds(half * u + side * h2, h2)]
            return remote(part, r2.at[half, side], ssem.at[0, half, side], q2.at[half, side], to(half, 0, 1 - 2 * side))

        def last_send(half, side):
            part = stages[3 + side].at[pl.ds(half * u, u)]
            return remote(part, r3.at[half, side], ssem.at[3 + side, half, 0], q3.at[half, side], to(half, 0, 1 - 2 * side))

        add(0, from_near(2))
        rounded(0, 0)
        for half in (0, 1):
            for side in (0, 1):
                turn_send(half, side).start()
        pending[0] = [(lambda half=half, side=side: turn_send(half, side)) for half in (0, 1) for side in (0, 1)]

        level1(0, (1, 2))

        for side in (0, 1):
            add(1 + side, from_near(1 - 2 * side))
        for side in (0, 1):
            add(
                1 + side,
                [(turn_send(half, side).wait_recv, r2.at[half, side], half * u + side * h2, h2) for half in (0, 1)],
            )
            rounded(1 + side, 3 + side)
            for half in (0, 1):
                last_send(half, side).start()
            pending[3 + side] = [(lambda half=half, side=side: last_send(half, side)) for half in (0, 1)]

        add(3, from_near(0))
        add(
            3,
            [
                (last_send(half, side).wait_recv, r3.at[half, side], half * u, u)
                for half in (0, 1)
                for side in (0, 1)
            ],
        )
        rounded(3, 0)
        out = pltpu.make_async_copy(stages[0], y, lsem.at[0])
        out.start()
        for stage in (1, 2, 3, 4):
            free(stage)
        out.wait()

    pl.run_scoped(
        scatter,
        pltpu.VMEM((4, 2 * u, depth), F32),
        pltpu.VMEM((2, h2, depth), BF16),
        pltpu.VMEM((4, u, depth), BF16),
        pltpu.VMEM((3, 2 * u, depth), BF16),
    )

    down.wait_send()
    for k in range(len(counts)):
        part = own(0).at[pl.ds(0, h2)] if k in halves_sent else own(0)
        remote(part, part, send.at[k], recv.at[0, 0], me.partner).wait_send()
    for half in (0, 1):
        for slot in range(len(ORDER)):
            remote(own(half), own(half), psend.at[half, slot], recv.at[0, 0], me.partner).wait_send()


def solution(mesh):
    n = math.isqrt(mesh.shape["tp"] // 2)
    assert n == 4 and 2 * n * n == mesh.shape["tp"]

    def step(x, w_gate, w_up, w_down):
        rows, depth = x.shape
        units = w_gate.shape[1]
        u = rows // 2
        dma = pltpu.SemaphoreType.DMA
        like = jax.ShapeDtypeStruct
        y, *_ = pl.pallas_call(
            functools.partial(kernel, n),
            out_shape=(
                like((rows, depth), BF16),
                like((2, 2, n, n, u, depth), BF16),
                like((2, 2, n, n, u, units), BF16),
                like((2, 2, n, u // 2, depth), BF16),
                like((2, 2, n, u, depth), BF16),
                like((2, 2, u // 2, depth), BF16),
                like((2, 2, u, depth), BF16),
            ),
            in_specs=[ANY] * 4,
            out_specs=(ANY,) * 7,
            scratch_shapes=[
                pltpu.VMEM((2 * units, depth), BF16),
                pltpu.VMEM((2, 2 * u, 2 * units), BF16),
                pltpu.VMEM((2, 2 * u, depth), BF16),
                dma((32,)),
                dma((2, 17)),
                dma((2, 16)),
                dma((2, 16)),
                dma((units // 128, 2)),
                dma((2, 2, 2)),
                dma((2, 2)),
                dma((2, 2)),
                dma((2, 16)),
                dma((3,)),
                dma((2, 2, 2)),
                dma((5, 2, 2)),
                dma((2, 2, n)),
                dma((2, 2, n)),
                dma((2, 2)),
                dma((2, 2)),
                dma((4,)),
            ],
            compiler_params=pltpu.CompilerParams(
                collective_id=0, has_side_effects=True, vmem_limit_bytes=LIMIT
            ),
            name="block",
        )(x, w_gate, w_up, w_down)
        return y

    return jax.shard_map(
        step,
        mesh=mesh,
        in_specs=(P(("dp", "tp"), None), P(None, "tp"), P(None, "tp"), P("tp", None)),
        out_specs=P(("dp", "tp"), None),
        check_vma=False,
    )
```
